512 devices in a mesh: fsdp: 64 (over x, y, core), dp: 8 (over z).
Axes of the slice: x: 4, y: 8, z: 8, core: 2. Of those that a mesh axis runs over, the one named last changes fastest.
Arguments:
- grads: bfloat16 [8, 1024, 28672], P('dp', 'fsdp')
- block_slot: int32 [28], replicated, may hold values from 0 to 63, as said below
- left_stats: float32 [64, 1024, 1024], P('fsdp', 'dp')
- right_stats: float32 [64, 1024, 1024], P('fsdp', 'dp')
- left_root: bfloat16 [64, 1024, 1024], P('fsdp', 'dp')
- right_root: bfloat16 [64, 1024, 1024], P('fsdp', 'dp')
Outputs:
- left_new: float32 [64, 1024, 1024], P('fsdp', 'dp')
- right_new: float32 [64, 1024, 1024], P('fsdp', 'dp')
- update: bfloat16 [1024, 28672], P('fsdp')
The draws below stay inside these ranges and needn't reach their ends.
Inputs may be any that keep to these rules, and one draw needn't show every extreme that they name: The entries of block_slot are distinct. Block b's statistics and roots sit in slot block_slot[b], which belongs to the fsdp device of index block_slot[b]; slots that no block names are empty and their statistics pass through unchanged.
All inputs are finite; a program needn't handle non-finite values.
Results may differ from the reference program's by a relative error of at most 0.015.
Values may be sent and summed in bfloat16 or wider, within the bound.
No kernel may reach another device: no remote copies, remote signals or barrier semaphores. Data moves between devices by JAX's collectives and lax.ppermute only.
A program may use at most 64 MiB of HBM per device.

```python
import math
import jax
import jax.numpy as jnp
from jax import lax

BLOCK = 1024
COLS = 28672
REPLICAS = 8
SLOTS = 1
SLOT_TOTAL = 64
N_FSDP = 64


def scaled_log(key, shape, low, high):
    return jnp.exp(jax.random.uniform(key, shape, jnp.float32, math.log(low), math.log(high)))


def draw_grads(key, part):
    keys = jax.random.split(jax.random.fold_in(key, 11), 3)
    row_scale = scaled_log(keys[0], (BLOCK,), 1.0, 4.0)
    col_scale = scaled_log(keys[1], (COLS,), 1.0, 4.0)
    noise = jax.random.normal(keys[2], (REPLICAS, BLOCK, COLS), jnp.float32)
    values = 0.004 * noise * row_scale[None, :, None] * col_scale[None, None, :]
    return values.astype(jnp.bfloat16)


def draw_block_slot(key, part):
    order = jax.random.permutation(jax.random.fold_in(key, 23), SLOT_TOTAL)
    return order[:COLS // BLOCK].astype(jnp.int32)


def definite(key, low, high, spread):
    keys = jax.random.split(key, 2)
    diagonal = scaled_log(keys[0], (SLOT_TOTAL, BLOCK), low, high)
    noise = jax.random.normal(keys[1], (SLOT_TOTAL, BLOCK, BLOCK), jnp.float32)
    symmetric = (noise + jnp.swapaxes(noise, 1, 2)) * (spread / math.sqrt(2.0 * BLOCK))
    return symmetric + diagonal[:, :, None] * jnp.eye(BLOCK, dtype=jnp.float32)[None]


def draw_left_stats(key, part):
    return definite(jax.random.fold_in(key, 31), 1.0, 4.0, 0.8)


def draw_right_stats(key, part):
    return definite(jax.random.fold_in(key, 37), 1.0, 4.0, 0.8)


def draw_left_root(key, part):
    return definite(jax.random.fold_in(key, 41), 0.5, 1.5, 0.3).astype(jnp.bfloat16)


def draw_right_root(key, part):
    return definite(jax.random.fold_in(key, 43), 0.5, 1.5, 0.3).astype(jnp.bfloat16)


def setup_inputs(seed: int = 0) -> dict:
    key_of = jax.random.split(jax.random.key(seed), 7)
    return {
        "grads": draw_grads(jax.random.fold_in(key_of[6], 71), 0),
        "block_slot": draw_block_slot(jax.random.fold_in(key_of[6], 71), 0),
        "left_stats": draw_left_stats(jax.random.fold_in(key_of[6], 71), 0),
        "right_stats": draw_right_stats(jax.random.fold_in(key_of[6], 71), 0),
        "left_root": draw_left_root(jax.random.fold_in(key_of[6], 71), 0),
        "right_root": draw_right_root(jax.random.fold_in(key_of[6], 71), 0),
    }


epsilon = 1e-06

def reference(grads, block_slot, left_stats, right_stats, left_root, right_root):
    block_count = COLS // BLOCK
    total_slots = SLOTS * N_FSDP
    summed = lax.optimization_barrier(jnp.sum(grads.astype(jnp.float32), axis=0)).astype(jnp.bfloat16)
    gradient = summed.reshape(BLOCK, block_count, BLOCK).transpose(1, 0, 2)
    numbers = jnp.arange(block_count, dtype=jnp.int32)

    def statistics(slot_id):
        matches = block_slot == slot_id
        filled = jnp.any(matches)
        position = jnp.sum(jnp.where(matches, numbers, 0)).astype(jnp.int32)
        chosen = jnp.where(filled, gradient[position], jnp.zeros((), jnp.bfloat16))
        left_sum = left_stats[slot_id] + jnp.dot(chosen, chosen.T, preferred_element_type=jnp.float32)
        right_sum = right_stats[slot_id] + jnp.dot(chosen.T, chosen, preferred_element_type=jnp.float32)
        return (left_sum, right_sum)
    left_new, right_new = lax.map(statistics, jnp.arange(total_slots, dtype=jnp.int32))

    def precondition(operands):
        one_block, slot_id = operands
        left_applied = jnp.dot(left_root[slot_id], one_block, preferred_element_type=jnp.float32).astype(jnp.bfloat16)
        both_applied = jnp.dot(left_applied, right_root[slot_id], preferred_element_type=jnp.float32)
        return (both_applied * lax.rsqrt(jnp.mean(both_applied * both_applied) + epsilon)).astype(jnp.bfloat16)
    updates = lax.map(precondition, (gradient, block_slot))
    update = updates.transpose(1, 0, 2).reshape(BLOCK, COLS)
    return (left_new, right_new, update)
```

```python
import jax
import jax.numpy as jnp
from jax import lax
from jax.sharding import Mesh
from jax.sharding import PartitionSpec as P

FSDP = ("fsdp_0", "fsdp_1", "fsdp_2")


epsilon = 1e-06


def per_device(grads, block_slot, left_stats, right_stats, left_root, right_root):
    rows = grads[0]
    row_dev, col_count = rows.shape
    block_size = left_stats.shape[2]
    block_count = col_count // block_size
    shared = left_stats.shape[1]
    replicas = lax.axis_size("dp")
    total_slots = lax.axis_size(FSDP)

    slot_ids = jnp.arange(total_slots, dtype=jnp.int32)
    matches = block_slot[None, :] == slot_ids[:, None]
    filled = jnp.any(matches, axis=1)
    numbers = jnp.arange(block_count, dtype=jnp.int32)
    source = jnp.sum(jnp.where(matches, numbers[None, :], 0), axis=1)

    whole_left = lax.all_gather(left_root[0], "dp", axis=0, tiled=True)

    shares = rows.reshape(row_dev, block_count, replicas, shared).transpose(2, 1, 0, 3)
    shares = shares.reshape(replicas, block_count * row_dev, shared)
    roots = right_root[0].reshape(shared, replicas, shared).transpose(1, 0, 2)
    message = jnp.concatenate([shares, roots], axis=1)
    received = lax.all_to_all(message, "dp", 0, 0, tiled=True)
    summed = jnp.sum(received[:, : block_count * row_dev].astype(jnp.float32), axis=0)
    summed = summed.astype(jnp.bfloat16).reshape(block_count, row_dev, shared)
    right_cols = received[:, block_count * row_dev :]

    outgoing = jnp.where(
        filled[:, None, None], jnp.take(summed, source, axis=0), jnp.zeros((), jnp.bfloat16)
    )
    incoming = lax.all_to_all(outgoing, FSDP, 0, 0, tiled=True)
    mine, whole_left = lax.optimization_barrier((incoming.reshape(block_size, shared), whole_left))
    gradient = lax.all_gather(mine, "dp", axis=1, tiled=True)

    inner = jnp.einsum(
        "rk,kc->rc",
        gradient,
        right_cols.reshape(block_size, shared),
        preferred_element_type=jnp.float32,
    )
    high = lax.reduce_precision(inner, 8, 7)
    low = (inner - high).astype(jnp.bfloat16)
    high = high.astype(jnp.bfloat16)
    both = jnp.einsum(
        "kr,rc->kc", whole_left, high, preferred_element_type=jnp.float32
    ) + jnp.einsum("kr,rc->kc", whole_left, low, preferred_element_type=jnp.float32)
    both = both.astype(jnp.bfloat16).reshape(total_slots, row_dev, shared)
    back = lax.all_to_all(both, FSDP, 0, 0, tiled=True)

    row_start = lax.axis_index("dp") * shared
    own_rows = lax.dynamic_slice_in_dim(gradient, row_start, shared, 0)
    left_new = left_stats + jnp.einsum(
        "rc,kc->rk", own_rows, gradient, preferred_element_type=jnp.float32
    )
    right_new = right_stats + jnp.einsum(
        "rc,rk->ck", mine, gradient, preferred_element_type=jnp.float32
    )

    wide = back.astype(jnp.float32)
    squares = lax.psum(jnp.sum(wide * wide, axis=(1, 2)), FSDP + ("dp",))
    picked = jnp.take(back, block_slot, axis=0)
    full = lax.all_gather(picked, "dp", axis=0, tiled=False)
    factor = lax.rsqrt(jnp.take(squares, block_slot) / (block_size * block_size) + epsilon)
    update = (full.astype(jnp.float32) * factor[None, :, None, None]).astype(jnp.bfloat16)
    update = update.transpose(2, 1, 0, 3).reshape(row_dev, col_count)
    return (left_new, right_new, update)


def solution(mesh):
    split = Mesh(
        mesh.devices.reshape(4, 8, 2, mesh.shape["dp"]), ("fsdp_0", "fsdp_1", "fsdp_2", "dp")
    )
    placed = (
        P("dp", FSDP, None),
        P(),
        P(FSDP, "dp", None),
        P(FSDP, "dp", None),
        P(FSDP, "dp", None),
        P(FSDP, "dp", None),
    )
    return jax.shard_map(
        per_device,
        mesh=split,
        in_specs=placed,
        out_specs=(P(FSDP, "dp", None), P(FSDP, "dp", None), P(FSDP, None)),
        check_vma=False,
    )
```

```python
import jax
import jax.numpy as jnp
from jax import lax
from jax.sharding import Mesh
from jax.sharding import PartitionSpec as P

FSDP = ("fsdp_0", "fsdp_1", "fsdp_2")


epsilon = 1e-06


def split_terms(value):
    high = lax.reduce_precision(value, 8, 7)
    middle = lax.reduce_precision(value - high, 8, 7)
    low = (value - high) - middle
    return [term.astype(jnp.bfloat16) for term in (high, middle, low)]


def per_device(grads, block_slot, left_stats, right_stats, left_root, right_root):
    rows = grads[0]
    row_dev, col_count = rows.shape
    block_size = left_stats.shape[2]
    block_count = col_count // block_size
    shared = left_stats.shape[1]
    replicas = lax.axis_size("dp")
    total_slots = lax.axis_size(FSDP)

    slot_ids = jnp.arange(total_slots, dtype=jnp.int32)
    matches = block_slot[None, :] == slot_ids[:, None]
    filled = jnp.any(matches, axis=1)
    numbers = jnp.arange(block_count, dtype=jnp.int32)
    source = jnp.sum(jnp.where(matches, numbers[None, :], 0), axis=1)

    whole_left = lax.all_gather(left_root[0], "dp", axis=0, tiled=True)

    shares = rows.reshape(row_dev, block_count, replicas, shared).transpose(2, 1, 0, 3)
    shares = shares.reshape(replicas, block_count * row_dev, shared)
    roots = right_root[0].reshape(shared, replicas, shared).transpose(1, 0, 2)
    message = jnp.concatenate([shares, roots], axis=1)
    received = lax.all_to_all(message, "dp", 0, 0, tiled=True)
    summed = jnp.sum(received[:, : block_count * row_dev].astype(jnp.float32), axis=0)
    summed = summed.astype(jnp.bfloat16).reshape(block_count, row_dev, shared)
    right_cols = received[:, block_count * row_dev :]

    outgoing = jnp.where(
        filled[:, None, None], jnp.take(summed, source, axis=0), jnp.zeros((), jnp.bfloat16)
    )
    incoming = lax.all_to_all(outgoing, FSDP, 0, 0, tiled=True)
    mine, whole_left = lax.optimization_barrier((incoming.reshape(block_size, shared), whole_left))
    gradient = lax.all_gather(mine, "dp", axis=1, tiled=True)

    inner = jnp.einsum(
        "rk,kc->rc",
        gradient,
        right_cols.reshape(block_size, shared),
        preferred_element_type=jnp.float32,
    )
    high = lax.reduce_precision(inner, 8, 7)
    low = (inner - high).astype(jnp.bfloat16)
    high = high.astype(jnp.bfloat16)
    both = jnp.einsum(
        "kr,rc->kc", whole_left, high, preferred_element_type=jnp.float32
    ) + jnp.einsum("kr,rc->kc", whole_left, low, preferred_element_type=jnp.float32)
    partial = split_terms(jnp.sum(both * both))
    lanes = jnp.concatenate([jnp.stack(partial), jnp.zeros(shared - 3, jnp.bfloat16)])
    marks = jnp.broadcast_to(lanes[None, None, :], (total_slots, 8, shared))
    both = both.astype(jnp.bfloat16).reshape(total_slots, row_dev, shared)
    back = lax.all_to_all(jnp.concatenate([both, marks], axis=1), FSDP, 0, 0, tiled=True)

    row_start = lax.axis_index("dp") * shared
    own_rows = lax.dynamic_slice_in_dim(gradient, row_start, shared, 0)
    left_new = left_stats + jnp.einsum(
        "rc,kc->rk", own_rows, gradient, preferred_element_type=jnp.float32
    )
    right_new = right_stats + jnp.einsum(
        "rc,rk->ck", mine, gradient, preferred_element_type=jnp.float32
    )

    picked = jnp.take(back, block_slot, axis=0)
    terms = jnp.zeros((32, shared), jnp.bfloat16).at[:block_count].set(picked[:, row_dev, :])
    tiles = picked[:, :row_dev].reshape(block_count * row_dev, shared)
    gathered = lax.all_gather(jnp.concatenate([tiles, terms]), "dp", axis=0, tiled=False)
    full = gathered[:, : block_count * row_dev].reshape(replicas, block_count, row_dev, shared)
    terms = gathered[:, block_count * row_dev :][:, :block_count, :3].astype(jnp.float32)
    squares = jnp.sum(terms, axis=(0, 2))
    factor = lax.rsqrt(squares / (block_size * block_size) + epsilon)
    update = (full.astype(jnp.float32) * factor[None, :, None, None]).astype(jnp.bfloat16)
    update = update.transpose(2, 1, 0, 3).reshape(row_dev, col_count)
    return (left_new, right_new, update)


def solution(mesh):
    split = Mesh(
        mesh.devices.reshape(4, 8, 2, mesh.shape["dp"]), ("fsdp_0", "fsdp_1", "fsdp_2", "dp")
    )
    placed = (
        P("dp", FSDP, None),
        P(),
        P(FSDP, "dp", None),
        P(FSDP, "dp", None),
        P(FSDP, "dp", None),
        P(FSDP, "dp", None),
    )
    return jax.shard_map(
        per_device,
        mesh=split,
        in_specs=placed,
        out_specs=(P(FSDP, "dp", None), P(FSDP, "dp", None), P(FSDP, None)),
        check_vma=False,
    )
```

```python
import functools

import jax
import jax.numpy as jnp
from jax import lax
from jax.experimental import pallas as pl
from jax.experimental.pallas import tpu as pltpu
from jax.sharding import Mesh
from jax.sharding import PartitionSpec as P


FSDP = ("fsdp_0", "fsdp_1", "fsdp_2")


epsilon = 1e-06
VMEM = pl.BlockSpec(memory_space=pltpu.VMEM)


def ring(array, axis, step):
    count = lax.axis_size(axis)
    return lax.ppermute(array, axis, [(i, (i + step) % count) for i in range(count)])


def offsets(count):
    return [0] + [-s for s in range(1, count // 2 + 1)] + list(range(1, (count + 1) // 2))


def ring_gather(array, axis):
    count = lax.axis_size(axis)
    up, down, ups, downs = array, array, [], []
    for s in range(1, count // 2 + 1):
        up = ring(up, axis, 1)
        ups.append(up)
        if s < (count + 1) // 2:
            down = ring(down, axis, -1)
            downs.append(down)
    return [array] + ups + downs


def dot(a, b, dims=((1,), (0,))):
    return lax.dot_general(a, b, (dims, ((), ())), preferred_element_type=jnp.float32)


def roots_kernel(count, left, right, *outs):
    me = lax.axis_index("dp")
    half = left.shape[0] // 2
    rows = right.shape[0] // 4
    width = right.shape[1] // 4
    for k, out in enumerate(outs):
        target = (me + k) % count
        upper = (target // 4) > 0
        start = pl.multiple_of((target % 4) * width, width)
        for f in range(half // 8):
            low, high = left[16 * f : 16 * f + 8, :], left[16 * f + 8 : 16 * f + 16, :]
            out[8 * f : 8 * f + 8, :] = jnp.where(upper, high, low)
        for g in range(4):
            out[half:, g * width : (g + 1) * width] = right[g * rows : (g + 1) * rows, pl.ds(start, width)]


def precondition_kernel(count, *refs):
    shards, roots, (out,) = refs[:count], refs[count : 2 * count], refs[2 * count :]
    me = lax.axis_index("dp")
    width = shards[0].shape[1]
    half = 64
    quarter = roots[0].shape[1] // 4

    def right(i):
        return [roots[i][half:, g * quarter : (g + 1) * quarter] for g in range(4)]

    inner = None
    for i in range(0, count, 2):
        pair = jnp.concatenate([shards[i][...], shards[i + 1][...]], axis=1)
        term = dot(pair, jnp.concatenate(right(i) + right(i + 1), axis=0))
        inner = term if inner is None else inner + term
    high = inner.astype(jnp.bfloat16)
    low = (inner - high.astype(jnp.float32)).astype(jnp.bfloat16)
    left = jnp.concatenate([root[:half, :] for root in roots], axis=0)
    both = dot(left, high) + dot(left, low)
    total = jnp.sum(jnp.sum(both * both, axis=0, keepdims=True), axis=1, keepdims=True)
    first = total.astype(jnp.bfloat16).astype(jnp.float32)
    second = (total - first).astype(jnp.bfloat16).astype(jnp.float32)
    third = (total - first) - second
    lane = lax.broadcasted_iota(jnp.int32, (8, width), 1)
    marks = jnp.where(lane == 0, first, jnp.where(lane == 1, second, jnp.where(lane == 2, third, 0.0)))
    for i, offset in enumerate(offsets(count)):
        start = ((me + offset + count) % count) * 8
        rows = both[i * half : (i + 1) * half]
        for part in range(2):
            tile = rows[:, part * width : (part + 1) * width].reshape(8, 8, width)
            out[pl.ds(start, 8), part * 8 : (part + 1) * 8, :] = tile.astype(jnp.bfloat16)
    out[:, 16:24, :] = jnp.broadcast_to(marks.astype(jnp.bfloat16)[None], (out.shape[0], 8, width))


def statistics_kernel(count, *refs):
    shards, (left, right, left_out, right_out) = refs[:count], refs[count:]
    me = lax.axis_index("dp")
    width = shards[0].shape[1]
    own = pl.multiple_of(me * width, width)
    total = left[0]
    for offset, shard in zip(offsets(count), shards):
        start = pl.multiple_of(((me + offset + count) % count) * width, width)
        total = total + dot(shard[pl.ds(own, width), :], shard[...], ((1,), (1,)))
        right_out[0, :, pl.ds(start, width)] = right[0, :, pl.ds(start, width)] + dot(
            shards[0][...], shard[...], ((0,), (0,))
        )
    left_out[0] = total


def step(grads, block_slot, left_stats, right_stats, left_root, right_root):
    rows = grads[0]
    row_dev, col_count = rows.shape
    block_size = left_stats.shape[2]
    block_count = col_count // block_size
    shared = left_stats.shape[1]
    replicas = lax.axis_size("dp")
    total_slots = lax.axis_size(FSDP)
    half_rows = row_dev // 2
    quarters = replicas // 2

    slot_ids = jnp.arange(total_slots, dtype=jnp.int32)
    matches = block_slot[None, :] == slot_ids[:, None]
    filled = jnp.any(matches, axis=1)
    numbers = jnp.arange(block_count, dtype=jnp.int32)
    source = jnp.sum(jnp.where(matches, numbers[None, :], 0), axis=1)

    shares = rows.reshape(row_dev, block_count, replicas, shared).transpose(2, 1, 0, 3)
    shares = shares.reshape(replicas, block_count * row_dev, shared)
    received = lax.all_to_all(shares, "dp", 0, 0, tiled=True)

    pieces = pl.pallas_call(
        functools.partial(roots_kernel, replicas),
        out_shape=[jax.ShapeDtypeStruct((3 * shared // 4, block_size), jnp.bfloat16)] * replicas,
        in_specs=[VMEM] * 2,
        out_specs=[VMEM] * replicas,
    )(left_root[0], right_root[0])
    arrived = {0: pieces[0]}
    for k in (4, 3, 5, 2, 6, 1, 7):
        arrived[k] = ring(pieces[k], "dp", k)
    roots = [arrived[-offset % replicas] for offset in offsets(replicas)]

    summed = jnp.sum(received.astype(jnp.float32), axis=0)
    summed = summed.astype(jnp.bfloat16).reshape(block_count, row_dev, shared)
    outgoing = jnp.where(
        filled[:, None, None], jnp.take(summed, source, axis=0), jnp.zeros((), jnp.bfloat16)
    )
    incoming = lax.all_to_all(outgoing, FSDP, 0, 0, tiled=True)
    shards = ring_gather(incoming.reshape(block_size, shared), "dp")

    message = pl.pallas_call(
        functools.partial(precondition_kernel, replicas),
        out_shape=jax.ShapeDtypeStruct((total_slots, row_dev + 8, shared), jnp.bfloat16),
        in_specs=[VMEM] * (2 * replicas),
        out_specs=VMEM,
    )(*shards, *roots)
    back = lax.all_to_all(message, FSDP, 0, 0, tiled=True)

    left_new, right_new = pl.pallas_call(
        functools.partial(statistics_kernel, replicas),
        out_shape=[jax.ShapeDtypeStruct(left_stats.shape, jnp.float32)] * 2,
        in_specs=[VMEM] * (replicas + 2),
        out_specs=[VMEM] * 2,
    )(*shards, left_stats, right_stats)

    picked = jnp.take(back, block_slot, axis=0)
    terms = jnp.zeros((32, shared), jnp.bfloat16).at[:block_count].set(picked[:, row_dev, :])
    tiles = picked[:, :row_dev].reshape(block_count * row_dev, shared)
    gathered = lax.all_gather(jnp.concatenate([tiles, terms]), "dp", axis=0, tiled=False)
    terms = gathered[:, block_count * row_dev :][:, :block_count, :3].astype(jnp.float32)
    squares = jnp.sum(terms, axis=(0, 2))
    factor = lax.rsqrt(squares / (block_size * block_size) + epsilon)
    full = gathered[:, : block_count * row_dev]
    full = full.reshape(2, quarters, block_count, 2, half_rows, shared).astype(jnp.float32)
    update = (full * factor[None, None, :, None, None, None]).astype(jnp.bfloat16)
    update = update.transpose(0, 4, 2, 1, 3, 5).reshape(row_dev, col_count)
    return (left_new, right_new, update)


def solution(mesh):
    split = Mesh(
        mesh.devices.reshape(4, 8, 2, mesh.shape["dp"]), ("fsdp_0", "fsdp_1", "fsdp_2", "dp")
    )
    placed = (
        P("dp", FSDP, None),
        P(),
        P(FSDP, "dp", None),
        P(FSDP, "dp", None),
        P(FSDP, "dp", None),
        P(FSDP, "dp", None),
    )
    return jax.shard_map(
        step,
        mesh=split,
        in_specs=placed,
        out_specs=(P(FSDP, "dp", None), P(FSDP, "dp", None), P(FSDP, None)),
        check_vma=False,
    )
```

```python
import functools

import jax
import jax.numpy as jnp
from jax import lax
from jax.experimental import pallas as pl
from jax.experimental.pallas import tpu as pltpu
from jax.sharding import Mesh
from jax.sharding import PartitionSpec as P


FSDP = ("fsdp_0", "fsdp_1", "fsdp_2")


epsilon = 1e-06
VMEM = pl.BlockSpec(memory_space=pltpu.VMEM)


def ring(array, axis, step):
    count = lax.axis_size(axis)
    return lax.ppermute(array, axis, [(i, (i + step) % count) for i in range(count)])


def offsets(count):
    return [0] + [-s for s in range(1, count // 2 + 1)] + list(range(1, (count + 1) // 2))


def ring_gather(array, axis):
    count = lax.axis_size(axis)
    up, down, ups, downs = array, array, [], []
    for s in range(1, count // 2 + 1):
        up = ring(up, axis, 1)
        ups.append(up)
        if s < (count + 1) // 2:
            down = ring(down, axis, -1)
            downs.append(down)
    return [array] + ups + downs


def dot(a, b, dims=((1,), (0,))):
    return lax.dot_general(a, b, (dims, ((), ())), preferred_element_type=jnp.float32)


def shares_kernel(rows, out):
    height, width = rows.shape[0], out.shape[2]
    for d in range(out.shape[0]):
        for b in range(out.shape[1] // height):
            start = (b * out.shape[0] + d) * width
            out[d, b * height : (b + 1) * height, :] = rows[:, start : start + width]


def roots_kernel(count, left, right, *outs):
    me = lax.axis_index("dp")
    half = left.shape[0] // 2
    rows = right.shape[0] // 4
    width = right.shape[1] // 4
    for k, out in enumerate(outs):
        target = (me + k) % count
        upper = (target // 4) > 0
        start = pl.multiple_of((target % 4) * width, width)
        for f in range(half // 8):
            low, high = left[16 * f : 16 * f + 8, :], left[16 * f + 8 : 16 * f + 16, :]
            out[8 * f : 8 * f + 8, :] = jnp.where(upper, high, low)
        for g in range(4):
            out[half:, g * width : (g + 1) * width] = right[g * rows : (g + 1) * rows, pl.ds(start, width)]


def precondition_kernel(count, *refs):
    sources, (out, shard_buffer, root_buffer, arrived) = refs[: 2 * count], refs[2 * count :]
    shards = [shard_buffer.at[i] for i in range(count)]
    roots = [root_buffer.at[i] for i in range(count)]
    copies = [
        pltpu.make_async_copy(source, target, arrived.at[i])
        for i, (source, target) in enumerate(zip(sources, shards + roots))
    ]
    for i in range(0, count, 2):
        for k in (i, i + 1, count + i, count + i + 1):
            copies[k].start()
    me = lax.axis_index("dp")
    width = shards[0].shape[1]
    half = roots[0].shape[0] * 2 // 3
    quarter = roots[0].shape[1] // 4

    def right(i):
        return [roots[i][half:, g * quarter : (g + 1) * quarter] for g in range(4)]

    inner = None
    for i in range(0, count, 2):
        for k in (i, i + 1, count + i, count + i + 1):
            copies[k].wait()
        pair = jnp.concatenate([shards[i][...], shards[i + 1][...]], axis=1)
        term = dot(pair, jnp.concatenate(right(i) + right(i + 1), axis=0))
        inner = term if inner is None else inner + term
    high = inner.astype(jnp.bfloat16)
    low = (inner - high.astype(jnp.float32)).astype(jnp.bfloat16)
    left = jnp.concatenate([root[:half, :] for root in roots], axis=0)
    both = dot(left, high) + dot(left, low)
    total = jnp.sum(jnp.sum(both * both, axis=0, keepdims=True), axis=1, keepdims=True)
    first = total.astype(jnp.bfloat16).astype(jnp.float32)
    second = (total - first).astype(jnp.bfloat16).astype(jnp.float32)
    third = (total - first) - second
    lane = lax.broadcasted_iota(jnp.int32, (8, width), 1)
    marks = jnp.where(lane == 0, first, jnp.where(lane == 1, second, jnp.where(lane == 2, third, 0.0)))
    for i, offset in enumerate(offsets(count)):
        start = ((me + offset + count) % count) * 8
        rows = both[i * half : (i + 1) * half]
        for part in range(2):
            tile = rows[:, part * width : (part + 1) * width].reshape(8, 8, width)
            out[pl.ds(start, 8), part * 8 : (part + 1) * 8, :] = tile.astype(jnp.bfloat16)
    out[:, 16:24, :] = jnp.broadcast_to(marks.astype(jnp.bfloat16)[None], (out.shape[0], 8, width))


def statistics_kernel(count, *refs):
    shards, (left, right, left_out, right_out) = refs[:count], refs[count:]
    me = lax.axis_index("dp")
    width = shards[0].shape[1]
    own = pl.multiple_of(me * width, width)
    total = left[0]
    for offset, shard in zip(offsets(count), shards):
        start = pl.multiple_of(((me + offset + count) % count) * width, width)
        total = total + dot(shard[pl.ds(own, width), :], shard[...], ((1,), (1,)))
        right_out[0, :, pl.ds(start, width)] = right[0, :, pl.ds(start, width)] + dot(
            shards[0][...], shard[...], ((0,), (0,))
        )
    left_out[0] = total


def step(grads, block_slot, left_stats, right_stats, left_root, right_root):
    rows = grads[0]
    row_dev, col_count = rows.shape
    block_size = left_stats.shape[2]
    block_count = col_count // block_size
    shared = left_stats.shape[1]
    replicas = lax.axis_size("dp")
    total_slots = lax.axis_size(FSDP)
    half_rows = row_dev // 2
    quarters = replicas // 2

    slot_ids = jnp.arange(total_slots, dtype=jnp.int32)
    matches = block_slot[None, :] == slot_ids[:, None]
    filled = jnp.any(matches, axis=1)
    numbers = jnp.arange(block_count, dtype=jnp.int32)
    source = jnp.sum(jnp.where(matches, numbers[None, :], 0), axis=1)

    groups = 4 if block_count % 4 == 0 else 1
    shares = pl.pallas_call(
        shares_kernel,
        grid=(groups,),
        out_shape=jax.ShapeDtypeStruct((replicas, block_count * row_dev, shared), jnp.bfloat16),
        in_specs=[pl.BlockSpec((row_dev, col_count // groups), lambda i: (0, i))],
        out_specs=pl.BlockSpec((replicas, block_count * row_dev // groups, shared), lambda i: (0, i, 0)),
    )(rows)
    received = lax.all_to_all(shares, "dp", 0, 0, tiled=True)

    pieces = pl.pallas_call(
        functools.partial(roots_kernel, replicas),
        out_shape=[jax.ShapeDtypeStruct((3 * shared // 4, block_size), jnp.bfloat16)] * replicas,
        in_specs=[VMEM] * 2,
        out_specs=[VMEM] * replicas,
    )(left_root[0], right_root[0])
    arrived = {0: pieces[0]}
    for k in (4, 3, 5, 2, 6, 1, 7):
        arrived[k] = ring(pieces[k], "dp", k)
    roots = [arrived[-offset % replicas] for offset in offsets(replicas)]

    summed = jnp.sum(received.astype(jnp.float32), axis=0)
    summed = summed.astype(jnp.bfloat16).reshape(block_count, row_dev, shared)
    outgoing = jnp.where(
        filled[:, None, None], jnp.take(summed, source, axis=0), jnp.zeros((), jnp.bfloat16)
    )
    incoming = lax.all_to_all(outgoing, FSDP, 0, 0, tiled=True)
    shards = ring_gather(incoming.reshape(block_size, shared), "dp")

    message = pl.pallas_call(
        functools.partial(precondition_kernel, replicas),
        out_shape=jax.ShapeDtypeStruct((total_slots, row_dev + 8, shared), jnp.bfloat16),
        in_specs=[pl.BlockSpec(memory_space=pl.ANY)] * (2 * replicas),
        out_specs=VMEM,
        scratch_shapes=[
            pltpu.VMEM((replicas,) + shards[0].shape, jnp.bfloat16),
            pltpu.VMEM((replicas,) + roots[0].shape, jnp.bfloat16),
            pltpu.SemaphoreType.DMA((2 * replicas,)),
        ],
    )(*shards, *roots)
    back = lax.all_to_all(message, FSDP, 0, 0, tiled=True)

    left_new, right_new = pl.pallas_call(
        functools.partial(statistics_kernel, replicas),
        out_shape=[jax.ShapeDtypeStruct(left_stats.shape, jnp.float32)] * 2,
        in_specs=[VMEM] * (replicas + 2),
        out_specs=[VMEM] * 2,
    )(*shards, left_stats, right_stats)

    picked = jnp.take(back, block_slot, axis=0)
    terms = jnp.zeros((32, shared), jnp.bfloat16).at[:block_count].set(picked[:, row_dev, :])
    tiles = picked[:, :row_dev].reshape(block_count * row_dev, shared)
    gathered = lax.all_gather(jnp.concatenate([tiles, terms]), "dp", axis=0, tiled=False)
    terms = gathered[:, block_count * row_dev :][:, :block_count, :3].astype(jnp.float32)
    squares = jnp.sum(terms, axis=(0, 2))
    factor = lax.rsqrt(squares / (block_size * block_size) + epsilon)
    full = gathered[:, : block_count * row_dev]
    full = full.reshape(2, quarters, block_count, 2, half_rows, shared).astype(jnp.float32)
    update = (full * factor[None, None, :, None, None, None]).astype(jnp.bfloat16)
    update = update.transpose(0, 4, 2, 1, 3, 5).reshape(row_dev, col_count)
    return (left_new, right_new, update)


def solution(mesh):
    split = Mesh(
        mesh.devices.reshape(4, 8, 2, mesh.shape["dp"]), ("fsdp_0", "fsdp_1", "fsdp_2", "dp")
    )
    placed = (
        P("dp", FSDP, None),
        P(),
        P(FSDP, "dp", None),
        P(FSDP, "dp", None),
        P(FSDP, "dp", None),
        P(FSDP, "dp", None),
    )
    return jax.shard_map(
        step,
        mesh=split,
        in_specs=placed,
        out_specs=(P(FSDP, "dp", None), P(FSDP, "dp", None), P(FSDP, None)),
        check_vma=False,
    )
```

```python
import functools

import jax
import jax.numpy as jnp
from jax import lax
from jax.experimental import pallas as pl
from jax.experimental.pallas import tpu as pltpu
from jax.sharding import Mesh
from jax.sharding import PartitionSpec as P


FSDP = ("fsdp_0", "fsdp_1", "fsdp_2")


epsilon = 1e-06
VMEM = pl.BlockSpec(memory_space=pltpu.VMEM)


def ring(array, axis, step):
    count = lax.axis_size(axis)
    return lax.ppermute(array, axis, [(i, (i + step) % count) for i in range(count)])


def offsets(count):
    half = count // 2
    return [0] + [sign * s for s in range(1, half) for sign in (-1, 1)] + [half]


def ring_gather(array, axis, cores):
    count = lax.axis_size(axis)
    half = count // 2
    up, down, shards = array, array, [array]
    for _ in range(1, half):
        up = ring(up, axis, 1)
        down = ring(down, axis, -1)
        shards += [up, down]
    last = jnp.where(lax.axis_index(cores) == 0, up, down)
    pairs = [(i, (i + 1) % count) for i in range(count)]
    pairs += [(count + i, count + (i - 1) % count) for i in range(count)]
    shards.append(lax.ppermute(last, (cores, axis), pairs))
    return shards


def dot(a, b, dims=((1,), (0,))):
    return lax.dot_general(a, b, (dims, ((), ())), preferred_element_type=jnp.float32)


def roots_kernel(count, left, right, *outs):
    me = lax.axis_index("dp")
    half = left.shape[0] // 2
    rows = right.shape[0] // 4
    width = right.shape[1] // 4
    for k, out in enumerate(outs):
        target = (me + k) % count
        upper = (target // 4) > 0
        start = pl.multiple_of((target % 4) * width, width)
        for f in range(half // 8):
            low, high = left[16 * f : 16 * f + 8, :], left[16 * f + 8 : 16 * f + 16, :]
            out[8 * f : 8 * f + 8, :] = jnp.where(upper, high, low)
        for g in range(4):
            out[half:, g * width : (g + 1) * width] = right[g * rows : (g + 1) * rows, pl.ds(start, width)]


def right_rows(root):
    half = root.shape[0] * 2 // 3
    quarter = root.shape[1] // 4
    return [root[half:, g * quarter : (g + 1) * quarter] for g in range(4)]


def inner_kernel(count, *refs):
    sources, (out, shard_buffer, root_buffer, arrived) = refs[: 2 * count], refs[2 * count :]
    shards = [shard_buffer.at[i] for i in range(count)]
    roots = [root_buffer.at[i] for i in range(count)]
    copies = [
        pltpu.make_async_copy(source, target, arrived.at[i])
        for i, (source, target) in enumerate(zip(sources, shards + roots))
    ]
    pairs = [tuple(range(i, min(i + 2, count))) for i in range(0, count, 2)]
    for pair in pairs:
        for i in pair:
            copies[i].start()
            copies[count + i].start()
    inner = None
    for pair in pairs:
        for i in pair:
            copies[i].wait()
            copies[count + i].wait()
        left = jnp.concatenate([shards[i][...] for i in pair], axis=1)
        term = dot(left, jnp.concatenate([r for i in pair for r in right_rows(roots[i])], axis=0))
        inner = term if inner is None else inner + term
    out[...] = inner


def precondition_kernel(count, *refs):
    inner_in, shard_in, sources = refs[0], refs[1], refs[2 : 2 + count]
    out, inner_buffer, shard_buffer, root_buffer, left, arrived = refs[2 + count :]
    half = left.shape[0] // count
    copies = [
        pltpu.make_async_copy(shard_in, shard_buffer, arrived.at[0]),
        pltpu.make_async_copy(sources[-1], root_buffer, arrived.at[1]),
        pltpu.make_async_copy(inner_in, inner_buffer, arrived.at[2]),
    ]
    for i in range(count):
        rows = left.at[i * half : (i + 1) * half]
        copies.append(pltpu.make_async_copy(sources[i].at[:half], rows, arrived.at[3 + i]))
    for copy in copies:
        copy.start()
    for copy in copies[:3]:
        copy.wait()
    me = lax.axis_index("dp")
    width = shard_buffer.shape[1]
    last = dot(shard_buffer[...], jnp.concatenate(right_rows(root_buffer), axis=0))
    inner = inner_buffer[...] + last
    high = inner.astype(jnp.bfloat16)
    low = (inner - high.astype(jnp.float32)).astype(jnp.bfloat16)
    for copy in copies[3:]:
        copy.wait()
    both = dot(left[...], high) + dot(left[...], low)
    total = jnp.sum(jnp.sum(both * both, axis=0, keepdims=True), axis=1, keepdims=True)
    first = total.astype(jnp.bfloat16).astype(jnp.float32)
    second = (total - first).astype(jnp.bfloat16).astype(jnp.float32)
    third = (total - first) - second
    lane = lax.broadcasted_iota(jnp.int32, (8, width), 1)
    marks = jnp.where(lane == 0, first, jnp.where(lane == 1, second, jnp.where(lane == 2, third, 0.0)))
    for i, offset in enumerate(offsets(count)):
        start = ((me + offset + count) % count) * 8
        rows = both[i * half : (i + 1) * half]
        for part in range(2):
            tile = rows[:, part * width : (part + 1) * width].reshape(8, 8, width)
            out[pl.ds(start, 8), part * 8 : (part + 1) * 8, :] = tile.astype(jnp.bfloat16)
    out[:, 16:24, :] = jnp.broadcast_to(marks.astype(jnp.bfloat16)[None], (out.shape[0], 8, width))


def statistics_kernel(count, *refs):
    shards, (left, right, left_out, right_out) = refs[:count], refs[count:]
    me = lax.axis_index("dp")
    width = shards[0].shape[1]
    own = pl.multiple_of(me * width, width)
    total = left[0]
    for offset, shard in zip(offsets(count), shards):
        start = pl.multiple_of(((me + offset + count) % count) * width, width)
        total = total + dot(shard[pl.ds(own, width), :], shard[...], ((1,), (1,)))
        right_out[0, :, pl.ds(start, width)] = right[0, :, pl.ds(start, width)] + dot(
            shards[0][...], shard[...], ((0,), (0,))
        )
    left_out[0] = total


def step(grads, block_slot, left_stats, right_stats, left_root, right_root):
    rows = grads[0]
    row_dev, col_count = rows.shape
    block_size = left_stats.shape[2]
    block_count = col_count // block_size
    shared = left_stats.shape[1]
    replicas = lax.axis_size("dp")
    total_slots = lax.axis_size(FSDP)
    half_rows = row_dev // 2
    quarters = replicas // 2

    slot_ids = jnp.arange(total_slots, dtype=jnp.int32)
    matches = block_slot[None, :] == slot_ids[:, None]
    numbers = jnp.arange(block_count, dtype=jnp.int32)
    source = block_count + jnp.sum(jnp.where(matches, numbers[None, :] - block_count, 0), axis=1)

    shares = rows.reshape(row_dev, block_count, replicas, shared).transpose(2, 1, 0, 3)
    shares = shares.reshape(replicas, block_count * row_dev, shared)
    received = lax.all_to_all(shares, "dp", 0, 0, tiled=True)

    pieces = pl.pallas_call(
        functools.partial(roots_kernel, replicas),
        out_shape=[jax.ShapeDtypeStruct((3 * shared // 4, block_size), jnp.bfloat16)] * replicas,
        in_specs=[VMEM] * 2,
        out_specs=[VMEM] * replicas,
    )(left_root[0], right_root[0])
    arrived = {0: pieces[0]}
    for k in (4, 3, 5, 2, 6, 1, 7):
        arrived[k] = ring(pieces[k], "dp", k)
    roots = [arrived[-offset % replicas] for offset in offsets(replicas)]

    summed = jnp.sum(received.astype(jnp.float32), axis=0)
    summed = summed.astype(jnp.bfloat16).reshape(block_count, row_dev, shared)
    summed = jnp.pad(summed, ((0, 4), (0, 0), (0, 0)))
    outgoing = summed.at[source].get(mode="promise_in_bounds")
    incoming = lax.all_to_all(outgoing, FSDP, 0, 0, tiled=True)
    shards = ring_gather(incoming.reshape(block_size, shared), "dp", FSDP[2])

    anywhere = pl.BlockSpec(memory_space=pl.ANY)
    before = replicas - 1
    quarter = block_size // quarters
    inner = pl.pallas_call(
        functools.partial(inner_kernel, before),
        out_shape=jax.ShapeDtypeStruct((block_size, quarter), jnp.float32),
        in_specs=[anywhere] * (2 * before),
        out_specs=VMEM,
        scratch_shapes=[
            pltpu.VMEM((before,) + shards[0].shape, jnp.bfloat16),
            pltpu.VMEM((before,) + roots[0].shape, jnp.bfloat16),
            pltpu.SemaphoreType.DMA((2 * before,)),
        ],
    )(*shards[:-1], *roots[:-1])
    message = pl.pallas_call(
        functools.partial(precondition_kernel, replicas),
        out_shape=jax.ShapeDtypeStruct((total_slots, row_dev + 8, shared), jnp.bfloat16),
        in_specs=[anywhere] * (2 + replicas),
        out_specs=VMEM,
        scratch_shapes=[
            pltpu.VMEM(inner.shape, jnp.float32),
            pltpu.VMEM(shards[0].shape, jnp.bfloat16),
            pltpu.VMEM(roots[0].shape, jnp.bfloat16),
            pltpu.VMEM((block_size // 2, block_size), jnp.bfloat16),
            pltpu.SemaphoreType.DMA((3 + replicas,)),
        ],
    )(inner, shards[-1], *roots)
    back = lax.all_to_all(message, FSDP, 0, 0, tiled=True)

    left_new, right_new = pl.pallas_call(
        functools.partial(statistics_kernel, replicas),
        out_shape=[jax.ShapeDtypeStruct(left_stats.shape, jnp.float32)] * 2,
        in_specs=[VMEM] * (replicas + 2),
        out_specs=[VMEM] * 2,
    )(*shards, left_stats, right_stats)

    picked = back.at[block_slot].get(mode="promise_in_bounds")
    terms = jnp.zeros((32, shared), jnp.bfloat16).at[:block_count].set(picked[:, row_dev, :])
    tiles = picked[:, :row_dev].reshape(block_count * row_dev, shared)
    gathered = lax.all_gather(jnp.concatenate([tiles, terms]), "dp", axis=0, tiled=False)
    terms = gathered[:, block_count * row_dev :][:, :block_count, :3].astype(jnp.float32)
    squares = jnp.sum(terms, axis=(0, 2))
    factor = lax.rsqrt(squares / (block_size * block_size) + epsilon)
    full = gathered[:, : block_count * row_dev]
    full = full.reshape(2, quarters, block_count, 2, half_rows, shared).astype(jnp.float32)
    update = (full * factor[None, None, :, None, None, None]).astype(jnp.bfloat16)
    update = update.transpose(0, 4, 2, 1, 3, 5).reshape(row_dev, col_count)
    return (left_new, right_new, update)


def solution(mesh):
    split = Mesh(
        mesh.devices.reshape(4, 8, 2, mesh.shape["dp"]), ("fsdp_0", "fsdp_1", "fsdp_2", "dp")
    )
    placed = (
        P("dp", FSDP, None),
        P(),
        P(FSDP, "dp", None),
        P(FSDP, "dp", None),
        P(FSDP, "dp", None),
        P(FSDP, "dp", None),
    )
    return jax.shard_map(
        step,
        mesh=split,
        in_specs=placed,
        out_specs=(P(FSDP, "dp", None), P(FSDP, "dp", None), P(FSDP, None)),
        check_vma=False,
    )
```

```python
import functools

import jax
import jax.numpy as jnp
from jax import lax
from jax.experimental import pallas as pl
from jax.experimental.pallas import tpu as pltpu
from jax.sharding import Mesh
from jax.sharding import PartitionSpec as P


FSDP = ("fsdp_0", "fsdp_1", "fsdp_2")


epsilon = 1e-06
VMEM = pl.BlockSpec(memory_space=pltpu.VMEM)


def ring(array, axis, step):
    count = lax.axis_size(axis)
    return lax.ppermute(array, axis, [(i, (i + step) % count) for i in range(count)])


def offsets(count):
    half = count // 2
    return [0] + [sign * s for s in range(1, half) for sign in (-1, 1)] + [half]


def ring_gather(array, axis):
    count = lax.axis_size(axis)
    half = count // 2
    up, down, shards = array, array, [array]
    for _ in range(1, half):
        up = ring(up, axis, 1)
        down = ring(down, axis, -1)
        shards += [up, down]
    shards.append(ring(up, axis, 1))
    return shards


def dot(a, b, dims=((1,), (0,))):
    return lax.dot_general(a, b, (dims, ((), ())), preferred_element_type=jnp.float32)


def roots_kernel(count, left, right, *outs):
    me = lax.axis_index("dp")
    half = left.shape[0] // 2
    rows = right.shape[0] // 4
    width = right.shape[1] // 4
    for k, out in enumerate(outs):
        target = (me + k) % count
        upper = (target // 4) > 0
        start = pl.multiple_of((target % 4) * width, width)
        for f in range(half // 8):
            low, high = left[16 * f : 16 * f + 8, :], left[16 * f + 8 : 16 * f + 16, :]
            out[8 * f : 8 * f + 8, :] = jnp.where(upper, high, low)
        for g in range(4):
            out[half:, g * width : (g + 1) * width] = right[g * rows : (g + 1) * rows, pl.ds(start, width)]


def right_rows(root):
    half = root.shape[0] * 2 // 3
    quarter = root.shape[1] // 4
    return [root[half:, g * quarter : (g + 1) * quarter] for g in range(4)]


def inner_kernel(count, *refs):
    sources, (out, shard_buffer, root_buffer, arrived) = refs[: 2 * count], refs[2 * count :]
    shards = [shard_buffer.at[i] for i in range(count)]
    roots = [root_buffer.at[i] for i in range(count)]
    copies = [
        pltpu.make_async_copy(source, target, arrived.at[i])
        for i, (source, target) in enumerate(zip(sources, shards + roots))
    ]
    pairs = [tuple(range(i, min(i + 2, count))) for i in range(0, count, 2)]
    for pair in pairs:
        for i in pair:
            copies[i].start()
            copies[count + i].start()
    inner = None
    for pair in pairs:
        for i in pair:
            copies[i].wait()
            copies[count + i].wait()
        left = jnp.concatenate([shards[i][...] for i in pair], axis=1)
        term = dot(left, jnp.concatenate([r for i in pair for r in right_rows(roots[i])], axis=0))
        inner = term if inner is None else inner + term
    out[...] = inner


def precondition_kernel(count, *refs):
    inner_in, shard_in, sources = refs[0], refs[1], refs[2 : 2 + count]
    out, inner_buffer, shard_buffer, root_buffer, left, arrived = refs[2 + count :]
    half = left.shape[0] // count
    copies = [
        pltpu.make_async_copy(shard_in, shard_buffer, arrived.at[0]),
        pltpu.make_async_copy(sources[-1], root_buffer, arrived.at[1]),
        pltpu.make_async_copy(inner_in, inner_buffer, arrived.at[2]),
    ]
    for i in range(count):
        rows = left.at[i * half : (i + 1) * half]
        copies.append(pltpu.make_async_copy(sources[i].at[:half], rows, arrived.at[3 + i]))
    for copy in copies:
        copy.start()
    for copy in copies[:3]:
        copy.wait()
    me = lax.axis_index("dp")
    width = shard_buffer.shape[1]
    last = dot(shard_buffer[...], jnp.concatenate(right_rows(root_buffer), axis=0))
    inner = inner_buffer[...] + last
    high = inner.astype(jnp.bfloat16)
    low = (inner - high.astype(jnp.float32)).astype(jnp.bfloat16)
    for copy in copies[3:]:
        copy.wait()
    both = dot(left[...], high) + dot(left[...], low)
    total = jnp.sum(jnp.sum(both * both, axis=0, keepdims=True), axis=1, keepdims=True)
    first = total.astype(jnp.bfloat16).astype(jnp.float32)
    second = (total - first).astype(jnp.bfloat16).astype(jnp.float32)
    third = (total - first) - second
    lane = lax.broadcasted_iota(jnp.int32, (8, width), 1)
    marks = jnp.where(lane == 0, first, jnp.where(lane == 1, second, jnp.where(lane == 2, third, 0.0)))
    for i, offset in enumerate(offsets(count)):
        start = ((me + offset + count) % count) * 8
        rows = both[i * half : (i + 1) * half]
        for part in range(2):
            tile = rows[:, part * width : (part + 1) * width].reshape(8, 8, width)
            out[pl.ds(start, 8), part * 8 : (part + 1) * 8, :] = tile.astype(jnp.bfloat16)
    out[:, 16:24, :] = jnp.broadcast_to(marks.astype(jnp.bfloat16)[None], (out.shape[0], 8, width))


def statistics_kernel(count, *refs):
    shards, (left, right, left_out, right_out) = refs[:count], refs[count:]
    me = lax.axis_index("dp")
    width = shards[0].shape[1]
    own = pl.multiple_of(me * width, width)
    total = left[0]
    for offset, shard in zip(offsets(count), shards):
        start = pl.multiple_of(((me + offset + count) % count) * width, width)
        total = total + dot(shard[pl.ds(own, width), :], shard[...], ((1,), (1,)))
        right_out[0, :, pl.ds(start, width)] = right[0, :, pl.ds(start, width)] + dot(
            shards[0][...], shard[...], ((0,), (0,))
        )
    left_out[0] = total


def step(grads, block_slot, left_stats, right_stats, left_root, right_root):
    rows = grads[0]
    row_dev, col_count = rows.shape
    block_size = left_stats.shape[2]
    block_count = col_count // block_size
    shared = left_stats.shape[1]
    replicas = lax.axis_size("dp")
    total_slots = lax.axis_size(FSDP)
    half_rows = row_dev // 2
    quarters = replicas // 2

    slot_ids = jnp.arange(total_slots, dtype=jnp.int32)
    matches = block_slot[None, :] == slot_ids[:, None]
    numbers = jnp.arange(block_count, dtype=jnp.int32)
    source = block_count + jnp.sum(jnp.where(matches, numbers[None, :] - block_count, 0), axis=1)

    shares = rows.reshape(row_dev, block_count, replicas, shared).transpose(2, 1, 0, 3)
    shares = shares.reshape(replicas, block_count * row_dev, shared)
    received = lax.all_to_all(shares, "dp", 0, 0, tiled=True)

    pieces = pl.pallas_call(
        functools.partial(roots_kernel, replicas),
        out_shape=[jax.ShapeDtypeStruct((3 * shared // 4, block_size), jnp.bfloat16)] * replicas,
        in_specs=[VMEM] * 2,
        out_specs=[VMEM] * replicas,
    )(left_root[0], right_root[0])
    arrived = {0: pieces[0]}
    for k in (4, 3, 5, 2, 6, 1, 7):
        arrived[k] = ring(pieces[k], "dp", k)
    roots = [arrived[-offset % replicas] for offset in offsets(replicas)]

    summed = jnp.sum(received.astype(jnp.float32), axis=0)
    summed = summed.astype(jnp.bfloat16).reshape(block_count, row_dev, shared)
    summed = jnp.pad(summed, ((0, 4), (0, 0), (0, 0)))
    outgoing = summed.at[source].get(mode="promise_in_bounds")
    incoming = lax.all_to_all(outgoing, FSDP, 0, 0, tiled=True)
    shards = ring_gather(incoming.reshape(block_size, shared), "dp")

    anywhere = pl.BlockSpec(memory_space=pl.ANY)
    before = replicas - 1
    quarter = block_size // quarters
    inner = pl.pallas_call(
        functools.partial(inner_kernel, before),
        out_shape=jax.ShapeDtypeStruct((block_size, quarter), jnp.float32),
        in_specs=[anywhere] * (2 * before),
        out_specs=VMEM,
        scratch_shapes=[
            pltpu.VMEM((before,) + shards[0].shape, jnp.bfloat16),
            pltpu.VMEM((before,) + roots[0].shape, jnp.bfloat16),
            pltpu.SemaphoreType.DMA((2 * before,)),
        ],
    )(*shards[:-1], *roots[:-1])
    message = pl.pallas_call(
        functools.partial(precondition_kernel, replicas),
        out_shape=jax.ShapeDtypeStruct((total_slots, row_dev + 8, shared), jnp.bfloat16),
        in_specs=[anywhere] * (2 + replicas),
        out_specs=VMEM,
        scratch_shapes=[
            pltpu.VMEM(inner.shape, jnp.float32),
            pltpu.VMEM(shards[0].shape, jnp.bfloat16),
            pltpu.VMEM(roots[0].shape, jnp.bfloat16),
            pltpu.VMEM((block_size // 2, block_size), jnp.bfloat16),
            pltpu.SemaphoreType.DMA((3 + replicas,)),
        ],
    )(inner, shards[-1], *roots)
    back = lax.all_to_all(message, FSDP, 0, 0, tiled=True)

    left_new, right_new = pl.pallas_call(
        functools.partial(statistics_kernel, replicas),
        out_shape=[jax.ShapeDtypeStruct(left_stats.shape, jnp.float32)] * 2,
        in_specs=[VMEM] * (replicas + 2),
        out_specs=[VMEM] * 2,
    )(*shards, left_stats, right_stats)

    picked = back.at[block_slot].get(mode="promise_in_bounds")
    terms = jnp.zeros((32, shared), jnp.bfloat16).at[:block_count].set(picked[:, row_dev, :])
    tiles = picked[:, :row_dev].reshape(block_count * row_dev, shared)
    gathered = lax.all_gather(jnp.concatenate([tiles, terms]), "dp", axis=0, tiled=False)
    terms = gathered[:, block_count * row_dev :][:, :block_count, :3].astype(jnp.float32)
    squares = jnp.sum(terms, axis=(0, 2))
    factor = lax.rsqrt(squares / (block_size * block_size) + epsilon)
    full = gathered[:, : block_count * row_dev]
    full = full.reshape(2, quarters, block_count, 2, half_rows, shared).astype(jnp.float32)
    update = (full * factor[None, None, :, None, None, None]).astype(jnp.bfloat16)
    update = update.transpose(0, 4, 2, 1, 3, 5).reshape(row_dev, col_count)
    return (left_new, right_new, update)


def solution(mesh):
    split = Mesh(
        mesh.devices.reshape(4, 8, 2, mesh.shape["dp"]), ("fsdp_0", "fsdp_1", "fsdp_2", "dp")
    )
    placed = (
        P("dp", FSDP, None),
        P(),
        P(FSDP, "dp", None),
        P(FSDP, "dp", None),
        P(FSDP, "dp", None),
        P(FSDP, "dp", None),
    )
    return jax.shard_map(
        step,
        mesh=split,
        in_specs=placed,
        out_specs=(P(FSDP, "dp", None), P(FSDP, "dp", None), P(FSDP, None)),
        check_vma=False,
    )
```

```python
import functools

import jax
import jax.numpy as jnp
from jax import lax
from jax.experimental import pallas as pl
from jax.experimental.pallas import tpu as pltpu
from jax.sharding import Mesh
from jax.sharding import PartitionSpec as P


FSDP = ("fsdp_0", "fsdp_1", "fsdp_2")


epsilon = 1e-06
VMEM = pl.BlockSpec(memory_space=pltpu.VMEM)


def ring(array, axis, step):
    count = lax.axis_size(axis)
    return lax.ppermute(array, axis, [(i, (i + step) % count) for i in range(count)])


def offsets(count):
    half = count // 2
    near = [sign * s for s in range(1, half) for sign in (-1, 1)]
    return [0] + near[1:] + [near[0], half]


def ring_gather(array, axis):
    count = lax.axis_size(axis)
    half = count // 2
    up, down, shards = array, array, [array]
    for _ in range(1, half):
        up = ring(up, axis, 1)
        down = ring(down, axis, -1)
        shards += [up, down]
    shards.append(ring(up, axis, 1))
    return shards[:1] + shards[2:-1] + [shards[1], shards[-1]]


def dot(a, b, dims=((1,), (0,))):
    return lax.dot_general(a, b, (dims, ((), ())), preferred_element_type=jnp.float32)


def roots_kernel(count, left, right, *outs):
    me = lax.axis_index("dp")
    half = left.shape[0] // 2
    rows = right.shape[0] // 4
    width = right.shape[1] // 4
    for k, out in enumerate(outs):
        target = (me + k) % count
        upper = (target // 4) > 0
        start = pl.multiple_of((target % 4) * width, width)
        for f in range(half // 8):
            low, high = left[16 * f : 16 * f + 8, :], left[16 * f + 8 : 16 * f + 16, :]
            out[8 * f : 8 * f + 8, :] = jnp.where(upper, high, low)
        for g in range(4):
            out[half:, g * width : (g + 1) * width] = right[g * rows : (g + 1) * rows, pl.ds(start, width)]


def right_rows(root):
    half = root.shape[0] * 2 // 3
    quarter = root.shape[1] // 4
    return [root[half:, g * quarter : (g + 1) * quarter] for g in range(4)]


def inner_kernel(count, *refs):
    sources, (out, shard_buffer, root_buffer, arrived) = refs[: 2 * count], refs[2 * count :]
    shards = [shard_buffer.at[i] for i in range(count)]
    roots = [root_buffer.at[i] for i in range(count)]
    copies = [
        pltpu.make_async_copy(source, target, arrived.at[i])
        for i, (source, target) in enumerate(zip(sources, shards + roots))
    ]
    pairs = [tuple(range(i, min(i + 2, count))) for i in range(0, count, 2)]
    for pair in pairs:
        for i in pair:
            copies[i].start()
            copies[count + i].start()
    inner = None
    for pair in pairs:
        for i in pair:
            copies[i].wait()
            copies[count + i].wait()
        left = jnp.concatenate([shards[i][...] for i in pair], axis=1)
        term = dot(left, jnp.concatenate([r for i in pair for r in right_rows(roots[i])], axis=0))
        inner = term if inner is None else inner + term
    out[...] = inner


def precondition_kernel(count, *refs):
    inner_in, shards_in, sources = refs[0], refs[1:3], refs[3 : 3 + count]
    out, inner_buffer, shard_buffer, root_buffer, left, arrived = refs[3 + count :]
    half = left.shape[0] // count
    late = list(zip(shards_in, [shard_buffer.at[i] for i in range(2)]))
    late += zip(sources[-2:], [root_buffer.at[i] for i in range(2)])
    late += [(inner_in, inner_buffer)]
    lefts = [(sources[i].at[:half], left.at[i * half : (i + 1) * half]) for i in range(count)]
    copies = [
        pltpu.make_async_copy(source, target, arrived.at[i])
        for i, (source, target) in enumerate(late + lefts)
    ]
    for copy in copies:
        copy.start()
    for copy in copies[:5]:
        copy.wait()
    me = lax.axis_index("dp")
    width = shard_buffer.shape[2]
    pair = jnp.concatenate([shard_buffer[i] for i in range(2)], axis=1)
    rights = [r for i in range(2) for r in right_rows(root_buffer.at[i])]
    last = dot(pair, jnp.concatenate(rights, axis=0))
    inner = inner_buffer[...] + last
    high = inner.astype(jnp.bfloat16)
    low = (inner - high.astype(jnp.float32)).astype(jnp.bfloat16)
    for copy in copies[5:]:
        copy.wait()
    both = dot(left[...], high) + dot(left[...], low)
    total = jnp.sum(jnp.sum(both * both, axis=0, keepdims=True), axis=1, keepdims=True)
    first = total.astype(jnp.bfloat16).astype(jnp.float32)
    second = (total - first).astype(jnp.bfloat16).astype(jnp.float32)
    third = (total - first) - second
    lane = lax.broadcasted_iota(jnp.int32, (8, width), 1)
    marks = jnp.where(lane == 0, first, jnp.where(lane == 1, second, jnp.where(lane == 2, third, 0.0)))
    for i, offset in enumerate(offsets(count)):
        start = ((me + offset + count) % count) * 8
        rows = both[i * half : (i + 1) * half]
        for part in range(2):
            tile = rows[:, part * width : (part + 1) * width].reshape(8, 8, width)
            out[pl.ds(start, 8), part * 8 : (part + 1) * 8, :] = tile.astype(jnp.bfloat16)
    out[:, 16:24, :] = jnp.broadcast_to(marks.astype(jnp.bfloat16)[None], (out.shape[0], 8, width))


def statistics_kernel(count, *refs):
    shards, (left, right, left_out, right_out) = refs[:count], refs[count:]
    me = lax.axis_index("dp")
    width = shards[0].shape[1]
    own = pl.multiple_of(me * width, width)
    total = left[0]
    for offset, shard in zip(offsets(count), shards):
        start = pl.multiple_of(((me + offset + count) % count) * width, width)
        total = total + dot(shard[pl.ds(own, width), :], shard[...], ((1,), (1,)))
        right_out[0, :, pl.ds(start, width)] = right[0, :, pl.ds(start, width)] + dot(
            shards[0][...], shard[...], ((0,), (0,))
        )
    left_out[0] = total


def step(grads, block_slot, left_stats, right_stats, left_root, right_root):
    rows = grads[0]
    row_dev, col_count = rows.shape
    block_size = left_stats.shape[2]
    block_count = col_count // block_size
    shared = left_stats.shape[1]
    replicas = lax.axis_size("dp")
    total_slots = lax.axis_size(FSDP)
    half_rows = row_dev // 2
    quarters = replicas // 2

    slot_ids = jnp.arange(total_slots, dtype=jnp.int32)
    matches = block_slot[None, :] == slot_ids[:, None]
    numbers = jnp.arange(block_count, dtype=jnp.int32)
    source = block_count + jnp.sum(jnp.where(matches, numbers[None, :] - block_count, 0), axis=1)

    shares = rows.reshape(row_dev, block_count, replicas, shared).transpose(2, 1, 0, 3)
    shares = shares.reshape(replicas, block_count * row_dev, shared)
    received = lax.all_to_all(shares, "dp", 0, 0, tiled=True)

    pieces = pl.pallas_call(
        functools.partial(roots_kernel, replicas),
        out_shape=[jax.ShapeDtypeStruct((3 * shared // 4, block_size), jnp.bfloat16)] * replicas,
        in_specs=[VMEM] * 2,
        out_specs=[VMEM] * replicas,
    )(left_root[0], right_root[0])
    arrived = {0: pieces[0]}
    for k in (4, 3, 5, 2, 6, 1, 7):
        arrived[k] = ring(pieces[k], "dp", k)
    roots = [arrived[-offset % replicas] for offset in offsets(replicas)]

    summed = jnp.sum(received.astype(jnp.float32), axis=0)
    summed = summed.astype(jnp.bfloat16).reshape(block_count, row_dev, shared)
    summed = jnp.pad(summed, ((0, 4), (0, 0), (0, 0)))
    outgoing = summed.at[source].get(mode="promise_in_bounds")
    incoming = lax.all_to_all(outgoing, FSDP, 0, 0, tiled=True)
    shards = ring_gather(incoming.reshape(block_size, shared), "dp")

    anywhere = pl.BlockSpec(memory_space=pl.ANY)
    before = replicas - 2
    quarter = block_size // quarters
    inner = pl.pallas_call(
        functools.partial(inner_kernel, before),
        out_shape=jax.ShapeDtypeStruct((block_size, quarter), jnp.float32),
        in_specs=[anywhere] * (2 * before),
        out_specs=VMEM,
        scratch_shapes=[
            pltpu.VMEM((before,) + shards[0].shape, jnp.bfloat16),
            pltpu.VMEM((before,) + roots[0].shape, jnp.bfloat16),
            pltpu.SemaphoreType.DMA((2 * before,)),
        ],
    )(*shards[:before], *roots[:before])
    message = pl.pallas_call(
        functools.partial(precondition_kernel, replicas),
        out_shape=jax.ShapeDtypeStruct((total_slots, row_dev + 8, shared), jnp.bfloat16),
        in_specs=[anywhere] * (3 + replicas),
        out_specs=VMEM,
        scratch_shapes=[
            pltpu.VMEM(inner.shape, jnp.float32),
            pltpu.VMEM((2,) + shards[0].shape, jnp.bfloat16),
            pltpu.VMEM((2,) + roots[0].shape, jnp.bfloat16),
            pltpu.VMEM((block_size // 2, block_size), jnp.bfloat16),
            pltpu.SemaphoreType.DMA((5 + replicas,)),
        ],
    )(inner, *shards[before:], *roots)
    back = lax.all_to_all(message, FSDP, 0, 0, tiled=True)

    left_new, right_new = pl.pallas_call(
        functools.partial(statistics_kernel, replicas),
        out_shape=[jax.ShapeDtypeStruct(left_stats.shape, jnp.float32)] * 2,
        in_specs=[VMEM] * (replicas + 2),
        out_specs=[VMEM] * 2,
    )(*shards, left_stats, right_stats)

    picked = back.at[block_slot].get(mode="promise_in_bounds")
    terms = jnp.zeros((32, shared), jnp.bfloat16).at[:block_count].set(picked[:, row_dev, :])
    tiles = picked[:, :row_dev].reshape(block_count * row_dev, shared)
    gathered = lax.all_gather(jnp.concatenate([tiles, terms]), "dp", axis=0, tiled=False)
    terms = gathered[:, block_count * row_dev :][:, :block_count, :3].astype(jnp.float32)
    squares = jnp.sum(terms, axis=(0, 2))
    factor = lax.rsqrt(squares / (block_size * block_size) + epsilon)
    full = gathered[:, : block_count * row_dev]
    full = full.reshape(2, quarters, block_count, 2, half_rows, shared).astype(jnp.float32)
    update = (full * factor[None, None, :, None, None, None]).astype(jnp.bfloat16)
    update = update.transpose(0, 4, 2, 1, 3, 5).reshape(row_dev, col_count)
    return (left_new, right_new, update)


def solution(mesh):
    split = Mesh(
        mesh.devices.reshape(4, 8, 2, mesh.shape["dp"]), ("fsdp_0", "fsdp_1", "fsdp_2", "dp")
    )
    placed = (
        P("dp", FSDP, None),
        P(),
        P(FSDP, "dp", None),
        P(FSDP, "dp", None),
        P(FSDP, "dp", None),
        P(FSDP, "dp", None),
    )
    return jax.shard_map(
        step,
        mesh=split,
        in_specs=placed,
        out_specs=(P(FSDP, "dp", None), P(FSDP, "dp", None), P(FSDP, None)),
        check_vma=False,
    )
```
